32 devices in a mesh: seq: 8 (over z, x), head: 4 (over y, core).
Axes of the slice: x: 2, y: 2, z: 4, core: 2. Of those that a mesh axis runs over, the one named last changes fastest.
Arguments:
- tokens: bfloat16 [2048, 4608], P('seq', 'head'), may hold values from -32 to 32
- segments: int32 [2048], P('seq'), may hold values from 0 to 7, never falling along the last dimension, each value on 1 to 1024 neighbouring positions
- pre_gain: float32 [4608], replicated, may hold values from 0.1 to 1.9
- post_gain: float32 [4608], replicated, may hold values from 0.1 to 1.9
- w_query: bfloat16 [4608, 1024], P('seq', 'head'), may hold values from -0.375 to 0.375
- w_key: bfloat16 [4608, 512], P('seq', 'head'), may hold values from -0.1875 to 0.1875
- w_value: bfloat16 [4608, 512], P('seq', 'head'), may hold values from -0.09375 to 0.09375
- w_out: bfloat16 [1024, 4608], P('head', 'seq'), may hold values from -0.1875 to 0.1875
Outputs:
- mixed: bfloat16 [2048, 4608], P('seq')
The draws below stay inside these ranges and needn't reach their ends.
Inputs may be any that keep to these rules, and one draw needn't show every extreme that they name: `segments`: segment ids never fall; each of the 8 documents holds at least one token and at most 1024, one exactly 1024.
All inputs are finite; a program needn't handle non-finite values.
Results may differ from the reference program's by a relative error of at most 0.01.
Values may be sent and summed in bfloat16 or wider, within the bound.
A program may use at most 64 MiB of HBM per device.

```python
import math
import jax
import jax.numpy as jnp
import numpy as np
from jax import lax

D = 4608
HD = 128
GROUP = 2
SCALAR = 144
DOCS = 8
KV_HEADS = 4
HEADS = 8
TOKENS = 2048
MOST = 1024
N_HEAD = 4


def draw_tokens(key, part):
    first, second, third = jax.random.split(jax.random.fold_in(key, 11), 3)
    base = jnp.clip(jax.random.normal(first, (TOKENS, D), jnp.float32), -4.0, 4.0)
    rows = jnp.exp(jax.random.uniform(second, (TOKENS, 1), jnp.float32, jnp.log(0.3), jnp.log(3.0)))
    cols = jnp.exp(jax.random.uniform(third, (1, D), jnp.float32, jnp.log(0.3), jnp.log(3.0)))
    return jnp.clip(base * rows * cols, -32.0, 32.0).astype(jnp.bfloat16)


def block_scale(rng, dims, pieces, least, high):
    level, own = 1.0, jax.random.fold_in(rng, 6)
    for axis_at, blocks in pieces:
        draws = jnp.exp(jax.random.uniform(jax.random.fold_in(own, axis_at), (blocks,), jnp.float32, least / len(pieces), high / len(pieces)))
        level = level * jnp.repeat(draws, dims[axis_at] // blocks).reshape([-1 if axis == axis_at else 1 for axis in range(len(dims))])
    return level


def profile(number_of, total, reach, lean):
    loads = [(1 << 20) // math.isqrt(grade ** lean) + 1 for grade in range(2, number_of + 1)]
    spare, given = total - reach - (number_of - 1), [1] * (number_of - 1)
    while spare > 0:
        free = [i for i in range(number_of - 1) if given[i] < reach]
        whole, budget = sum([loads[i] for i in free]), spare
        for i in free:
            extra = min(reach - given[i], max(1, budget * loads[i] // whole), spare)
            given[i] = given[i] + extra
            spare = spare - extra
    return np.array([reach] + given)


def ragged(rng, number_of, total, reach, lean):
    if number_of == 2:
        one = jax.random.randint(rng, (), max(1, total - reach), min(reach, total - 1) + 1)
        return jnp.stack([one, total - one])
    tallies = jnp.asarray(profile(number_of, total, reach, lean), jnp.int32)
    couples = (number_of - 1) // 2
    giver, taker = tallies[1:1 + 2 * couples:2], tallies[2:2 + 2 * couples:2]
    margin = jnp.minimum(giver - 1, reach - taker)
    passed = jax.random.randint(jax.random.fold_in(rng, 1), (couples,), 0, 1 << 20) % (margin + 1)
    tallies = tallies.at[1:1 + 2 * couples:2].set(giver - passed).at[2:2 + 2 * couples:2].set(taker + passed)
    return tallies[jax.random.permutation(jax.random.fold_in(rng, 2), number_of)]


def centred(own_key, dims, scale, limit, shards=(), held_as=jnp.bfloat16):
    values = jax.random.normal(own_key, dims, jnp.float32) * scale
    if len(shards) > 0:
        values = block_scale(own_key, dims, shards, -0.22, 0.18) * values
    return jnp.clip(values, min=-limit, max=limit).astype(held_as)


def setup_inputs(seed: int = 0) -> dict:
    key_list = jax.random.split(jax.random.key(seed), 9)
    return {
        "tokens": draw_tokens(jax.random.fold_in(key_list[8], 71), 0),
        "segments": jnp.searchsorted(jnp.cumsum(ragged(key_list[1], DOCS, TOKENS, MOST, 2)), jnp.arange(TOKENS), side="right").astype(jnp.int32),
        "pre_gain": jnp.clip(1.0 + 0.18 * jax.random.normal(key_list[2], (D,), jnp.float32), 0.1, 1.9),
        "post_gain": jnp.clip(1.0 + 0.18 * jax.random.normal(key_list[3], (D,), jnp.float32), 0.1, 1.9),
        "w_query": centred(key_list[4], (D, HEADS * HD), (D // 16) ** -0.5, 0.375, ((0, 8), (1, 4))),
        "w_key": centred(key_list[5], (D, KV_HEADS * HD), (D // 4) ** -0.5, 0.1875, ((0, 8), (1, 4))),
        "w_value": centred(key_list[6], (D, KV_HEADS * HD), D ** -0.5, 0.09375, ((0, 8), (1, 4))),
        "w_out": centred(key_list[7], (HEADS * HD, D), (HEADS * HD) ** -0.5, 0.1875, ((0, 4), (1, 8))),
    }


EPS = 1e-06
CAP = 50.0

def rotate(values, position, width):
    count = values.shape[1] // width
    half = width // 2
    shaped = values.reshape(values.shape[0], count, width)
    freq = 10000.0 ** (-(jnp.arange(half, dtype=jnp.float32) / half))
    angle = position[:, None] * freq[None, :]
    cosine = jnp.cos(angle)[:, None, :]
    sine = jnp.sin(angle)[:, None, :]
    first = shaped[:, :, :half]
    second = shaped[:, :, half:]
    turned = jnp.concatenate([first * cosine - second * sine, second * cosine + first * sine], axis=2)
    return turned.reshape(values.shape[0], count * width)

def reference(tokens, segments, pre_gain, post_gain, w_query, w_key, w_value, w_out):
    wide = tokens.astype(jnp.float32)
    normed = (wide * lax.rsqrt(lax.optimization_barrier(jnp.mean(wide * wide, axis=1, keepdims=True)) + EPS) * pre_gain).astype(jnp.bfloat16)
    query = jnp.dot(normed, w_query, preferred_element_type=jnp.float32)
    key_proj = jnp.dot(normed, w_key, preferred_element_type=jnp.float32)
    value_proj = jnp.dot(normed, w_value, preferred_element_type=jnp.float32)
    levels = jnp.arange(DOCS, dtype=jnp.int32)
    onehot = (segments[:, None] == levels[None, :]).astype(jnp.float32)
    counts = lax.optimization_barrier(jnp.sum(onehot, axis=0))
    before = jnp.cumsum(counts) - counts
    start = lax.optimization_barrier(jnp.sum(onehot * before[None, :], axis=1))
    index_f = jnp.arange(TOKENS, dtype=jnp.int32).astype(jnp.float32)
    position = index_f - start
    heads = HEADS
    kv_count = KV_HEADS
    rq = (rotate(query, position, HD) * SCALAR ** (-0.5)).astype(jnp.bfloat16)
    rq = rq.reshape(TOKENS, heads, HD).transpose(1, 0, 2)
    rk = rotate(key_proj, position, HD).astype(jnp.bfloat16).reshape(TOKENS, kv_count, HD).transpose(1, 0, 2)
    vb = value_proj.astype(jnp.bfloat16).reshape(TOKENS, kv_count, HD).transpose(1, 0, 2)
    allowed = (index_f[None, :] >= start[:, None]) & (index_f[None, :] <= index_f[:, None])

    def head_attn(head):
        qh = rq[head]
        kh = rk[head // GROUP]
        vh = vb[head // GROUP]
        scores = jnp.dot(qh, kh.T, preferred_element_type=jnp.float32)
        capped = CAP * jnp.tanh(scores / CAP)
        weights = jnp.where(allowed, jnp.exp(capped), 0.0)
        total = jnp.dot(weights.astype(jnp.bfloat16), vh, preferred_element_type=jnp.float32)
        return (total / lax.optimization_barrier(jnp.sum(weights, axis=1))[:, None]).astype(jnp.bfloat16)
    attn = lax.map(head_attn, jnp.arange(heads, dtype=jnp.int32))
    attn = attn.transpose(1, 0, 2).reshape(TOKENS, heads * HD)
    per = heads * HD // N_HEAD
    groups = attn.reshape(TOKENS, N_HEAD, per).transpose(1, 0, 2)
    out_groups = w_out.reshape(N_HEAD, per, D)

    def add_group(total, pair):
        part = jnp.dot(pair[0], pair[1], preferred_element_type=jnp.float32).astype(jnp.bfloat16)
        part = lax.optimization_barrier(part).astype(jnp.float32)
        return (total + part, None)
    proj, unused = lax.scan(add_group, jnp.zeros((TOKENS, D), jnp.float32), (groups, out_groups))
    scale = lax.rsqrt(lax.optimization_barrier(jnp.mean(proj * proj, axis=1, keepdims=True)) + EPS)
    return (wide + proj * scale * post_gain).astype(jnp.bfloat16)
```

```python
import functools

import jax
import jax.numpy as jnp
from jax import lax
from jax.experimental import pallas as pl
from jax.experimental.pallas import tpu as pltpu
from jax.sharding import PartitionSpec as P

HD = 128
GROUP = 2
SCALAR = 144
DOCS = 8


EPS = 1e-06
CAP = 50.0


def carried_in(value, axis, join, neutral):
    count, mine = (lax.axis_size(axis), lax.axis_index(axis))
    pieces = lax.all_gather(value, axis)
    subtotal = jnp.full_like(value, 0) + jnp.asarray(neutral, value.dtype)

    def step(position, subtotal):
        longer = join(subtotal, pieces[position])
        return jnp.where(position < mine, longer, subtotal)

    return lax.fori_loop(0, count - 1, step, subtotal)


def rotate(values, position, width):
    count = values.shape[1] // width
    half = width // 2
    shaped = values.reshape(values.shape[0], count, width)
    freq = 10000.0 ** (-(jnp.arange(half, dtype=jnp.float32) / half))
    angle = position[:, None] * freq[None, :]
    cosine = jnp.cos(angle)[:, None, :]
    sine = jnp.sin(angle)[:, None, :]
    first = shaped[:, :, :half]
    second = shaped[:, :, half:]
    turned = jnp.concatenate(
        [first * cosine - second * sine, second * cosine + first * sine], axis=2
    )
    return turned.reshape(values.shape[0], count * width)


def add_counts(earlier, later):
    return earlier + later


def local(tokens, segments, pre_gain, post_gain, w_query, w_key, w_value, w_out):
    rows = tokens.shape[0]
    whole = lax.all_gather(tokens, "head", axis=1, tiled=True)
    wide = whole.astype(jnp.float32)
    normed = (
        wide * lax.rsqrt(jnp.mean(wide * wide, axis=1, keepdims=True) + EPS) * pre_gain
    ).astype(jnp.bfloat16)
    pieces = (
        lax.all_gather(w_query, "seq", axis=0, tiled=True),
        lax.all_gather(w_key, "seq", axis=0, tiled=True),
        lax.all_gather(w_value, "seq", axis=0, tiled=True),
    )
    query, key_proj, value_proj = tuple(
        (jnp.dot(normed, piece, preferred_element_type=jnp.float32) for piece in pieces)
    )
    levels = jnp.arange(DOCS, dtype=jnp.int32)
    below = jnp.sum((levels[None, :] > segments[:, None]).astype(jnp.float32), axis=0)
    earlier = carried_in(below, "seq", add_counts, jnp.zeros((DOCS,), jnp.float32))
    starts = earlier + below
    onehot = (segments[:, None] == levels[None, :]).astype(jnp.float32)
    tok_start = jnp.sum(onehot * starts[None, :], axis=1)
    offset = lax.axis_index("seq") * rows
    index_f = (offset + jnp.arange(rows, dtype=jnp.int32)).astype(jnp.float32)
    position = index_f - tok_start
    kv_count = w_key.shape[1] // HD
    rq = (rotate(query, position, HD) * SCALAR ** (-0.5)).astype(jnp.bfloat16)
    rk = rotate(key_proj, position, HD).astype(jnp.bfloat16)
    vb = value_proj.astype(jnp.bfloat16)
    stacked = (
        rq.reshape(rows, kv_count, GROUP, HD)
        .transpose(1, 2, 0, 3)
        .reshape(kv_count, GROUP * rows, HD)
    )
    query_start = jnp.tile(tok_start, GROUP)
    query_index = jnp.tile(index_f, GROUP)
    empty = (
        jnp.zeros((kv_count, GROUP * rows, HD), jnp.float32),
        jnp.zeros((kv_count, GROUP * rows), jnp.float32),
    )
    keys_all = lax.all_gather(rk, "seq", axis=0, tiled=True)
    values_all = lax.all_gather(vb, "seq", axis=0, tiled=True)
    count = keys_all.shape[0]
    block = 1024
    steps_total = count // block

    def compute(offset_blk, state):
        numer, denom = state
        keys_blk = lax.dynamic_slice_in_dim(keys_all, offset_blk, block, 0).reshape(
            block, kv_count, HD
        )
        values_blk = lax.dynamic_slice_in_dim(values_all, offset_blk, block, 0).reshape(
            block, kv_count, HD
        )
        key_index = (offset_blk + jnp.arange(block, dtype=jnp.int32)).astype(jnp.float32)
        scores = jnp.einsum("cqd,kcd->cqk", stacked, keys_blk, preferred_element_type=jnp.float32)
        capped = CAP * jnp.tanh(scores / CAP)
        allowed = (key_index[None, None, :] >= query_start[None, :, None]) & (
            key_index[None, None, :] <= query_index[None, :, None]
        )
        weights = jnp.where(allowed, jnp.exp(capped), 0.0)
        numer = numer + jnp.einsum(
            "cqk,kcd->cqd",
            weights.astype(jnp.bfloat16),
            values_blk,
            preferred_element_type=jnp.float32,
        )
        denom = denom + jnp.sum(weights, axis=2)
        return (numer, denom)

    def one_block(step, state):
        offset_blk = step * block
        return compute(offset_blk, state)

    numer, denom = lax.fori_loop(0, steps_total, one_block, empty)
    attn = (numer / denom[:, :, None]).reshape(kv_count, GROUP, rows, HD).transpose(2, 0, 1, 3)
    attn = attn.reshape(rows, kv_count * GROUP * HD).astype(jnp.bfloat16)
    partial_proj = jnp.dot(
        attn, lax.all_gather(w_out, "seq", axis=1, tiled=True), preferred_element_type=jnp.float32
    )
    partial_proj = lax.optimization_barrier(partial_proj.astype(jnp.bfloat16)).astype(jnp.float32)
    summed = lax.psum(partial_proj.astype(jnp.bfloat16), "head").astype(jnp.float32)
    scale = lax.rsqrt(jnp.mean(summed * summed, axis=1, keepdims=True) + EPS)
    return (wide + summed * scale * post_gain).astype(jnp.bfloat16)


MESH = pl.DeviceIdType.MESH
BF16 = jnp.bfloat16
F32 = jnp.float32


def fits(mesh, tokens, w_key, w_out):
    seq, head = mesh.shape["seq"], mesh.shape["head"]
    width = tokens[1]
    lanes = -(-(width // seq) // 128) * 128
    weights = 2 * width * (w_key[1] // head) * (GROUP + 2)
    outs = 2 * w_out[0] * lanes * seq
    rows = tokens[0] // seq
    rest = rows * width * (2 + 2 + 4 + 2) + tokens[0] * (w_key[1] // head) * 4
    return (
        seq % 2 == 0
        and seq > 2
        and head % 2 == 0
        and seq % head == 0
        and w_key[1] // head == HD
        and (width // head) % 128 == 0
        and weights + outs + rest < 40 * 2**20
    )


class Line:
    def __init__(self, ref, recv, send, seq, down=True):
        self.ref, self.recv, self.send, self.down = ref, recv, send, down
        self.count = seq // 2
        me = lax.axis_index("seq")
        self.z, self.x = me // 2, lax.rem(me, 2)
        self.head = lax.axis_index("head")
        self.me = me

    def copy(self, block, way):
        target = (
            2 * (self.z + 1) + self.x,
            2 * (self.z - 1) + self.x,
            2 * self.z + 1 - self.x,
        )[way]
        return pltpu.make_async_remote_copy(
            src_ref=self.ref(block),
            dst_ref=self.ref(block),
            send_sem=self.send.at[way, block],
            recv_sem=self.recv.at[block],
            device_id=(target, self.head),
            device_id_type=MESH,
        )

    def up(self, block):
        @pl.when(self.z < self.count - 1)
        def _():
            self.copy(block, 0).start()

    def below(self, block):
        if self.down:

            @pl.when(self.z > 0)
            def _():
                self.copy(block, 1).start()

    def across(self, block):
        self.copy(block, 2).start()

    def wait(self, block):
        self.copy(block, 2).wait_recv()

    def step(self, k, also=None):
        @pl.when(self.z - k >= 0)
        def _():
            block = 2 * (self.z - k) + self.x
            self.wait(block)
            self.up(block)
            self.across(block)
            if also is not None:
                also(block)

        if self.down:

            @pl.when(self.z + k < self.count)
            def _():
                block = 2 * (self.z + k) + self.x
                self.wait(block)
                self.below(block)
                self.across(block)
                if also is not None:
                    also(block)

    def pairs(self, also=None):
        for z in range(self.count):
            block = 2 * z + 1 - self.x

            def take():
                self.wait(block)
                if also is not None:
                    also(block)

            if self.down:
                take()
            else:
                pl.when(z <= self.z)(take)

    def drain(self):
        for z in range(self.count):
            block = 2 * z + self.x

            def sent():
                self.copy(block, 2).wait_send()

            if self.down:
                sent()

                @pl.when((self.z > 0) & (z >= self.z))
                def _():
                    self.copy(block, 1).wait_send()
            else:
                pl.when(z <= self.z)(sent)

            @pl.when((self.z < self.count - 1) & (z <= self.z))
            def _():
                self.copy(block, 0).wait_send()


def kernel(
    seq, heads, rows, width,
    tok, seg_row, wq, wk, wv, wo_in, seg_col, pre, post, freq,
    out,
    X, XN, W, WO, SEG, KV, ATT, PR, ACC, RQ, NUM, DEN,
    loc, x_recv, x_send, x_core, s_recv, s_send, w_recv, w_send,
    o_recv, o_send, o_y, o_core, k_recv, k_send, a_recv, a_send, a_core,
):
    me, head = lax.axis_index("seq"), lax.axis_index("head")
    z, x = me // 2, lax.rem(me, 2)
    y, core = head // 2, lax.rem(head, 2)
    ys, line = heads // 2, seq // 2
    partner = 2 * y + 1 - core
    deep = width // seq
    cut = width // heads
    mates = [2 * lax.rem(y + d, ys) + core for d in range(1, ys)]

    moves = [
        pltpu.make_async_copy(seg_row, SEG.at[me], loc.at[0]),
        pltpu.make_async_copy(tok, X.at[head], loc.at[1]),
    ]
    mine = W.at[pl.ds(pl.multiple_of(me * deep, 16), deep)]
    kd = wk.shape[1]
    qd = wq.shape[1]
    moves += [
        pltpu.make_async_copy(wq, mine.at[:, pl.ds(0, qd)], loc.at[2]),
        pltpu.make_async_copy(wk, mine.at[:, pl.ds(qd, kd)], loc.at[3]),
        pltpu.make_async_copy(wv, mine.at[:, pl.ds(qd + kd, kd)], loc.at[4]),
        pltpu.make_async_copy(wo_in, WO.at[me, head], loc.at[5]),
    ]
    for move in moves:
        move.start()

    barrier = pltpu.get_barrier_semaphore()

    def greet(where):
        pl.semaphore_signal(barrier, inc=1, device_id=where, device_id_type=MESH)

    greet((2 * z + 1 - x, head))
    greet((me, partner))
    for mate in mates:
        greet((me, mate))

    @pl.when(z > 0)
    def _():
        greet((me - 2, head))

    @pl.when(z < line - 1)
    def _():
        greet((me + 2, head))

    ends = (z > 0).astype(jnp.int32) + (z < line - 1).astype(jnp.int32)
    pl.semaphore_wait(barrier, 2 + len(mates) + ends)

    for move in moves:
        move.wait()

    def sent_to(ref, send, recv, where):
        return pltpu.make_async_remote_copy(
            src_ref=ref, dst_ref=ref, send_sem=send, recv_sem=recv,
            device_id=where, device_id_type=MESH,
        )

    def x_copy(h, to, send):
        return sent_to(X.at[h], send, x_recv.at[h], (me, to))

    def a_copy(h, to, send):
        return sent_to(ATT.at[h], send, a_recv.at[h], (me, to))

    def o_copy(b, h, to, send):
        return sent_to(WO.at[b, h], send, o_recv.at[b, h], (me, to))

    segs = Line(lambda b: SEG.at[b], s_recv, s_send, seq)
    ws = Line(lambda b: W.at[pl.ds(pl.multiple_of(b * deep, 16), deep)], w_recv, w_send, seq)
    kvs = Line(lambda b: KV.at[b], k_recv, k_send, seq, down=False)
    wos = Line(lambda b: WO.at[b, head], o_recv.at[:, head], o_send, seq)

    def share(b):
        for d, mate in enumerate(mates):
            o_copy(b, head, mate, o_y.at[d, b]).start()
        o_copy(b, head, partner, o_core.at[b, y]).start()

    def begin(stream):
        stream.up(me)
        stream.below(me)
        stream.across(me)

    begin(segs)
    for d, mate in enumerate(mates):
        x_copy(head, mate, x_send.at[d]).start()
    x_copy(head, partner, x_core.at[y]).start()
    begin(ws)
    share(me)

    for k in range(1, line):
        segs.step(k)
        ws.step(k)
        if k == 1:
            for mate in mates:
                x_copy(mate, partner, x_core.at[mate // 2]).wait_recv()
                x_copy(mate, partner, x_core.at[mate // 2]).start()
            wos.up(me)
            wos.below(me)
        if k == line - 1:
            wos.across(me)
    for other in range(ys):
        x_copy(2 * other + 1 - core, partner, x_core.at[other]).wait_recv()

    half = rows // 2

    def norm_rows(r, _):
        at = pl.ds(pl.multiple_of(r * half, half), half)
        total = jnp.zeros((half, 1), F32)
        for h in range(heads):
            wide = X[h, at, :].astype(F32)
            total += jnp.sum(wide * wide, axis=1, keepdims=True)
        scale = lax.rsqrt(total / width + EPS)
        for h in range(heads):
            XN[h, at, :] = (X[h, at, :].astype(F32) * scale * pre[h]).astype(BF16)
        return 0

    lax.fori_loop(0, 2, norm_rows, 0)
    segs.pairs()
    col = seg_col[...]
    start = jnp.zeros((rows, 1), F32)
    for j in range(seq):
        start += jnp.sum((SEG[j, 0:1, :] < col).astype(F32), axis=1, keepdims=True)
    index = (me * rows + lax.broadcasted_iota(jnp.int32, (rows, 1), 0)).astype(F32)
    angle = (index - start) * freq[...]
    cosine = jnp.cos(angle)
    sine = jnp.sin(angle)
    lane = lax.broadcasted_iota(jnp.int32, (rows, HD), 1)
    sine = jnp.where(lane < HD // 2, -sine, sine)
    ws.pairs()

    ACC[...] = jnp.zeros_like(ACC)

    def project(h, _):
        part = W[pl.ds(pl.multiple_of(h * cut, 128), cut), :]
        ACC[...] += jnp.dot(XN[h], part, preferred_element_type=F32)
        return 0

    lax.fori_loop(0, heads, project, 0)

    def turn(values):
        return values * cosine + pltpu.roll(values, HD // 2, 1) * sine

    for g in range(GROUP):
        RQ[g * rows : (g + 1) * rows, :] = (
            turn(ACC[:, g * HD : (g + 1) * HD]) * SCALAR ** (-0.5)
        ).astype(BF16)
    KV[me, :, 0:HD] = turn(ACC[:, qd : qd + HD]).astype(BF16)
    KV[me, :, HD : 2 * HD] = ACC[:, qd + kd : qd + kd + HD].astype(BF16)
    begin(kvs)
    for k in range(1, line):
        kvs.step(k)
        wos.step(k, share)
    kvs.pairs()

    start2 = jnp.concatenate([start] * GROUP, axis=0)
    index2 = jnp.concatenate([index] * GROUP, axis=0)
    NUM[...] = jnp.zeros_like(NUM)
    DEN[...] = jnp.zeros_like(DEN)

    def attend(j, _):
        s = lax.dot_general(
            RQ[...], KV[j, :, 0:HD], (((1,), (1,)), ((), ())), preferred_element_type=F32
        )
        at = (j * rows + lax.broadcasted_iota(jnp.int32, (1, rows), 1)).astype(F32)
        p = jnp.where(
            (at >= start2) & (at <= index2), jnp.exp(CAP * jnp.tanh(s * (1.0 / CAP))), 0.0
        )
        DEN[...] += jnp.sum(p, axis=1, keepdims=True)
        NUM[...] += jnp.dot(p.astype(BF16), KV[j, :, HD : 2 * HD], preferred_element_type=F32)
        return 0

    lax.fori_loop(0, me + 1, attend, 0)
    ratio = (NUM[...] / DEN[:, 0:1]).astype(BF16)
    for g in range(GROUP):
        ATT[head, :, g * HD : (g + 1) * HD] = ratio[g * rows : (g + 1) * rows, :]
    for d, mate in enumerate(mates):
        a_copy(head, mate, a_send.at[d]).start()
    a_copy(head, partner, a_core.at[y]).start()

    wos.pairs(share)
    for mate in mates:
        a_copy(mate, partner, a_core.at[mate // 2]).wait_recv()
        a_copy(mate, partner, a_core.at[mate // 2]).start()
    for b in range(seq):
        for mate in mates:
            o_copy(b, mate, partner, o_core.at[b, mate // 2]).wait_recv()
            o_copy(b, mate, partner, o_core.at[b, mate // 2]).start()
    for other in range(ys):
        a_copy(2 * other + 1 - core, partner, a_core.at[other]).wait_recv()
    for b in range(seq):
        for other in range(ys):
            o_copy(b, 2 * other + 1 - core, partner, o_core.at[b, other]).wait_recv()

    def emit(b, total):
        acc = jnp.zeros((rows, deep), F32)
        for h in range(heads):
            acc += (
                jnp.dot(ATT[h], WO[b, h], preferred_element_type=F32).astype(BF16).astype(F32)
            )
        PR[b] = acc
        return total + jnp.sum(acc * acc, axis=1, keepdims=True)

    total = lax.fori_loop(0, seq, emit, jnp.zeros((rows, 1), F32))
    scale = lax.rsqrt(total / width + EPS)
    per = seq // heads

    def finish(h, _):
        wide = X[h].astype(F32)
        parts = [PR[h * per + i] for i in range(per)]
        proj = jnp.concatenate(parts, axis=1)
        at = pl.ds(pl.multiple_of(h * cut, 128), cut)
        out[:, at] = (wide + proj * scale * post[h]).astype(BF16)
        return 0

    lax.fori_loop(0, heads, finish, 0)

    for stream in (segs, ws, kvs, wos):
        stream.drain()
    for d, mate in enumerate(mates):
        x_copy(head, mate, x_send.at[d]).wait_send()
        a_copy(head, mate, a_send.at[d]).wait_send()
    for other in range(ys):
        x_copy(2 * other + core, partner, x_core.at[other]).wait_send()
        a_copy(2 * other + core, partner, a_core.at[other]).wait_send()
    for b in range(seq):
        for d, mate in enumerate(mates):
            o_copy(b, head, mate, o_y.at[d, b]).wait_send()
        for other in range(ys):
            o_copy(b, 2 * other + core, partner, o_core.at[b, other]).wait_send()


def fused(tokens, segments, pre_gain, post_gain, w_query, w_key, w_value, w_out):
    seq, heads = lax.axis_size("seq"), lax.axis_size("head")
    rows, cut = tokens.shape
    width = cut * heads
    deep = width // seq
    qd, kd = w_query.shape[1], w_key.shape[1]
    half = HD // 2
    freq = 10000.0 ** (-(jnp.arange(half, dtype=F32) / half))
    freq = jnp.concatenate([freq, freq])[None, :]
    hbm = pl.BlockSpec(memory_space=pl.ANY)
    vmem = pl.BlockSpec(memory_space=pltpu.VMEM)
    dma = pltpu.SemaphoreType.DMA
    ys = heads // 2
    return pl.pallas_call(
        functools.partial(kernel, seq, heads, rows, width),
        out_shape=jax.ShapeDtypeStruct((rows, width), BF16),
        in_specs=[hbm] * 6 + [vmem] * 4,
        out_specs=vmem,
        scratch_shapes=[
            pltpu.VMEM((heads, rows, cut), BF16),
            pltpu.VMEM((heads, rows, cut), BF16),
            pltpu.VMEM((width, qd + 2 * kd), BF16),
            pltpu.VMEM((seq, heads, w_out.shape[0], deep), BF16),
            pltpu.VMEM((seq, 8, rows), jnp.int32),
            pltpu.VMEM((seq, rows, 2 * HD), BF16),
            pltpu.VMEM((heads, rows, GROUP * HD), BF16),
            pltpu.VMEM((seq, rows, deep), F32),
            pltpu.VMEM((rows, qd + 2 * kd), F32),
            pltpu.VMEM((GROUP * rows, HD), BF16),
            pltpu.VMEM((GROUP * rows, HD), F32),
            pltpu.VMEM((GROUP * rows, HD), F32),
            dma((6,)),
            dma((heads,)), dma((max(ys - 1, 1),)), dma((ys,)),
            dma((seq,)), dma((3, seq)),
            dma((seq,)), dma((3, seq)),
            dma((seq, heads)), dma((3, seq)), dma((max(ys - 1, 1), seq)), dma((seq, ys)),
            dma((seq,)), dma((3, seq)),
            dma((heads,)), dma((max(ys - 1, 1),)), dma((ys,)),
        ],
        compiler_params=pltpu.CompilerParams(
            collective_id=0, has_side_effects=True, vmem_limit_bytes=60 * 2**20
        ),
    )(
        tokens, jnp.broadcast_to(segments[None, :], (8, rows)), w_query, w_key, w_value, w_out,
        segments[:, None], pre_gain.reshape(heads, 1, cut), post_gain.reshape(heads, 1, cut), freq,
    )


def solution(mesh):
    specs = (
        P("seq", "head"),
        P("seq"),
        P(),
        P(),
        P("seq", "head"),
        P("seq", "head"),
        P("seq", "head"),
        P("head", "seq"),
    )

    def run(*args):
        small = fits(mesh, args[0].shape, args[5].shape, args[7].shape)
        return jax.shard_map(
            fused if small else local,
            mesh=mesh,
            in_specs=specs,
            out_specs=P("seq", None),
            check_vma=False,
        )(*args)

    return run
```

```python
import functools

import jax
import jax.numpy as jnp
import numpy as np
from jax import lax
from jax.experimental import pallas as pl
from jax.experimental.pallas import tpu as pltpu
from jax.sharding import PartitionSpec as P

HD = 128
GROUP = 2
SCALAR = 144
DOCS = 8


EPS = 1e-06
CAP = 50.0


def carried_in(value, axis, join, neutral):
    count, mine = (lax.axis_size(axis), lax.axis_index(axis))
    pieces = lax.all_gather(value, axis)
    subtotal = jnp.full_like(value, 0) + jnp.asarray(neutral, value.dtype)

    def step(position, subtotal):
        longer = join(subtotal, pieces[position])
        return jnp.where(position < mine, longer, subtotal)

    return lax.fori_loop(0, count - 1, step, subtotal)


def rotate(values, position, width):
    count = values.shape[1] // width
    half = width // 2
    shaped = values.reshape(values.shape[0], count, width)
    freq = 10000.0 ** (-(jnp.arange(half, dtype=jnp.float32) / half))
    angle = position[:, None] * freq[None, :]
    cosine = jnp.cos(angle)[:, None, :]
    sine = jnp.sin(angle)[:, None, :]
    first = shaped[:, :, :half]
    second = shaped[:, :, half:]
    turned = jnp.concatenate(
        [first * cosine - second * sine, second * cosine + first * sine], axis=2
    )
    return turned.reshape(values.shape[0], count * width)


def add_counts(earlier, later):
    return earlier + later


def local(tokens, segments, pre_gain, post_gain, w_query, w_key, w_value, w_out):
    rows = tokens.shape[0]
    whole = lax.all_gather(tokens, "head", axis=1, tiled=True)
    wide = whole.astype(jnp.float32)
    normed = (
        wide * lax.rsqrt(jnp.mean(wide * wide, axis=1, keepdims=True) + EPS) * pre_gain
    ).astype(jnp.bfloat16)
    pieces = (
        lax.all_gather(w_query, "seq", axis=0, tiled=True),
        lax.all_gather(w_key, "seq", axis=0, tiled=True),
        lax.all_gather(w_value, "seq", axis=0, tiled=True),
    )
    query, key_proj, value_proj = tuple(
        (jnp.dot(normed, piece, preferred_element_type=jnp.float32) for piece in pieces)
    )
    levels = jnp.arange(DOCS, dtype=jnp.int32)
    below = jnp.sum((levels[None, :] > segments[:, None]).astype(jnp.float32), axis=0)
    earlier = carried_in(below, "seq", add_counts, jnp.zeros((DOCS,), jnp.float32))
    starts = earlier + below
    onehot = (segments[:, None] == levels[None, :]).astype(jnp.float32)
    tok_start = jnp.sum(onehot * starts[None, :], axis=1)
    offset = lax.axis_index("seq") * rows
    index_f = (offset + jnp.arange(rows, dtype=jnp.int32)).astype(jnp.float32)
    position = index_f - tok_start
    kv_count = w_key.shape[1] // HD
    rq = (rotate(query, position, HD) * SCALAR ** (-0.5)).astype(jnp.bfloat16)
    rk = rotate(key_proj, position, HD).astype(jnp.bfloat16)
    vb = value_proj.astype(jnp.bfloat16)
    stacked = (
        rq.reshape(rows, kv_count, GROUP, HD)
        .transpose(1, 2, 0, 3)
        .reshape(kv_count, GROUP * rows, HD)
    )
    query_start = jnp.tile(tok_start, GROUP)
    query_index = jnp.tile(index_f, GROUP)
    empty = (
        jnp.zeros((kv_count, GROUP * rows, HD), jnp.float32),
        jnp.zeros((kv_count, GROUP * rows), jnp.float32),
    )
    keys_all = lax.all_gather(rk, "seq", axis=0, tiled=True)
    values_all = lax.all_gather(vb, "seq", axis=0, tiled=True)
    count = keys_all.shape[0]
    block = 1024
    steps_total = count // block

    def compute(offset_blk, state):
        numer, denom = state
        keys_blk = lax.dynamic_slice_in_dim(keys_all, offset_blk, block, 0).reshape(
            block, kv_count, HD
        )
        values_blk = lax.dynamic_slice_in_dim(values_all, offset_blk, block, 0).reshape(
            block, kv_count, HD
        )
        key_index = (offset_blk + jnp.arange(block, dtype=jnp.int32)).astype(jnp.float32)
        scores = jnp.einsum("cqd,kcd->cqk", stacked, keys_blk, preferred_element_type=jnp.float32)
        capped = CAP * jnp.tanh(scores / CAP)
        allowed = (key_index[None, None, :] >= query_start[None, :, None]) & (
            key_index[None, None, :] <= query_index[None, :, None]
        )
        weights = jnp.where(allowed, jnp.exp(capped), 0.0)
        numer = numer + jnp.einsum(
            "cqk,kcd->cqd",
            weights.astype(jnp.bfloat16),
            values_blk,
            preferred_element_type=jnp.float32,
        )
        denom = denom + jnp.sum(weights, axis=2)
        return (numer, denom)

    def one_block(step, state):
        offset_blk = step * block
        return compute(offset_blk, state)

    numer, denom = lax.fori_loop(0, steps_total, one_block, empty)
    attn = (numer / denom[:, :, None]).reshape(kv_count, GROUP, rows, HD).transpose(2, 0, 1, 3)
    attn = attn.reshape(rows, kv_count * GROUP * HD).astype(jnp.bfloat16)
    partial_proj = jnp.dot(
        attn, lax.all_gather(w_out, "seq", axis=1, tiled=True), preferred_element_type=jnp.float32
    )
    partial_proj = lax.optimization_barrier(partial_proj.astype(jnp.bfloat16)).astype(jnp.float32)
    summed = lax.psum(partial_proj.astype(jnp.bfloat16), "head").astype(jnp.float32)
    scale = lax.rsqrt(jnp.mean(summed * summed, axis=1, keepdims=True) + EPS)
    return (wide + summed * scale * post_gain).astype(jnp.bfloat16)


MESH = pl.DeviceIdType.MESH
BF16 = jnp.bfloat16
F32 = jnp.float32


def fits(mesh, tokens, w_key, w_out):
    seq, head = mesh.shape["seq"], mesh.shape["head"]
    width = tokens[1]
    weights = 2 * width * (w_key[1] // head) * (GROUP + 2)
    outs = 2 * w_out[0] * width
    rows = tokens[0] // seq
    rest = rows * width * (2 + 2 + 4 + 2) + tokens[0] * (w_key[1] // head) * 4
    return (
        seq % 2 == 0
        and seq > 2
        and head % 2 == 0
        and seq % head == 0
        and w_key[1] // head == HD
        and (width // head) % 128 == 0
        and weights + outs + rest < 40 * 2**20
    )


class Line:
    def __init__(self, ref, recv, send, seq, down=True):
        self.ref, self.recv, self.send, self.down = ref, recv, send, down
        self.count = seq // 2
        me = lax.axis_index("seq")
        self.z, self.x = me // 2, lax.rem(me, 2)
        self.head = lax.axis_index("head")
        self.me = me

    def copy(self, block, way):
        target = (
            2 * (self.z + 1) + self.x,
            2 * (self.z - 1) + self.x,
            2 * self.z + 1 - self.x,
        )[way]
        return pltpu.make_async_remote_copy(
            src_ref=self.ref(block),
            dst_ref=self.ref(block),
            send_sem=self.send.at[way, block],
            recv_sem=self.recv.at[block],
            device_id=(target, self.head),
            device_id_type=MESH,
        )

    def up(self, block):
        @pl.when(self.z < self.count - 1)
        def _():
            self.copy(block, 0).start()

    def below(self, block):
        if self.down:

            @pl.when(self.z > 0)
            def _():
                self.copy(block, 1).start()

    def across(self, block):
        self.copy(block, 2).start()

    def wait(self, block):
        self.copy(block, 2).wait_recv()

    def at(self, k, act):
        @pl.when(self.z - k >= 0)
        def _():
            act(2 * (self.z - k) + self.x, self.up)

        if self.down:

            @pl.when(self.z + k < self.count)
            def _():
                act(2 * (self.z + k) + self.x, self.below)

    def near(self, k, also):
        def act(block, onward):
            self.wait(block)
            onward(block)
            also(block)

        self.at(k, act)

    def far(self, k):
        self.at(k, lambda block, onward: self.across(block))

    def step(self, k):
        self.near(k, self.across)

    def pairs(self, also=None, first=0, last=None):
        for away in range(first, self.count if last is None else last):
            z = lax.rem(self.z + away, self.count)
            block = 2 * z + 1 - self.x

            def take():
                self.wait(block)
                if also is not None:
                    also(block)

            if self.down:
                take()
            else:
                pl.when(z <= self.z)(take)

    def drain(self):
        for z in range(self.count):
            block = 2 * z + self.x

            def sent():
                self.copy(block, 2).wait_send()

            if self.down:
                sent()

                @pl.when((self.z > 0) & (z >= self.z))
                def _():
                    self.copy(block, 1).wait_send()
            else:
                pl.when(z <= self.z)(sent)

            @pl.when((self.z < self.count - 1) & (z <= self.z))
            def _():
                self.copy(block, 0).wait_send()


def kernel(
    seq, heads, rows, width,
    tok, seg_row, wq, wk, wv, wo_in, pre_in, post_in, freq_in,
    out,
    X, XN, W, WO, SEG, KV, ATT, PR, ACC, RQ, NUM, DEN, pre, post, freq,
    loc, x_recv, x_send, x_core, s_recv, s_send, w_recv, w_send,
    o_recv, o_send, o_y, o_core, k_recv, k_send, a_recv, a_send, a_core,
):
    me, head = lax.axis_index("seq"), lax.axis_index("head")
    z, x = me // 2, lax.rem(me, 2)
    y, core = head // 2, lax.rem(head, 2)
    ys, line = heads // 2, seq // 2
    partner = 2 * y + 1 - core
    deep = width // seq
    cut = width // heads
    mates = [2 * lax.rem(y + d, ys) + core for d in range(1, ys)]

    moves = [
        pltpu.make_async_copy(seg_row, SEG.at[me], loc.at[0]),
        pltpu.make_async_copy(tok, X.at[head], loc.at[1]),
    ]
    mine = W.at[pl.ds(pl.multiple_of(me * deep, 16), deep)]
    kd = wk.shape[1]
    qd = wq.shape[1]
    moves += [
        pltpu.make_async_copy(wq, mine.at[:, pl.ds(0, qd)], loc.at[2]),
        pltpu.make_async_copy(wk, mine.at[:, pl.ds(qd, kd)], loc.at[3]),
        pltpu.make_async_copy(wv, mine.at[:, pl.ds(qd + kd, kd)], loc.at[4]),
        pltpu.make_async_copy(
            wo_in, WO.at[head, pl.ds(pl.multiple_of(me * deep, 16), deep)], loc.at[5]
        ),
    ]
    small = [
        pltpu.make_async_copy(pre_in, pre, loc.at[6]),
        pltpu.make_async_copy(post_in, post, loc.at[7]),
        pltpu.make_async_copy(freq_in, freq, loc.at[8]),
    ]
    for move in small:
        move.start()
    for move in moves:
        move.start()

    barrier = pltpu.get_barrier_semaphore()

    def greet(where):
        pl.semaphore_signal(barrier, inc=1, device_id=where, device_id_type=MESH)

    greet((2 * z + 1 - x, head))
    greet((me, partner))
    for mate in mates:
        greet((me, mate))

    @pl.when(z > 0)
    def _():
        greet((me - 2, head))

    @pl.when(z < line - 1)
    def _():
        greet((me + 2, head))

    ends = (z > 0).astype(jnp.int32) + (z < line - 1).astype(jnp.int32)
    pl.semaphore_wait(barrier, 2 + len(mates) + ends)

    for move in moves:
        move.wait()

    def sent_to(ref, send, recv, where):
        return pltpu.make_async_remote_copy(
            src_ref=ref, dst_ref=ref, send_sem=send, recv_sem=recv,
            device_id=where, device_id_type=MESH,
        )

    def x_copy(h, to, send):
        return sent_to(X.at[h], send, x_recv.at[h], (me, to))

    def a_copy(h, to, send):
        return sent_to(ATT.at[h], send, a_recv.at[h], (me, to))

    def o_block(b, h):
        return WO.at[h, pl.ds(pl.multiple_of(b * deep, 16), deep)]

    def o_copy(b, h, to, send):
        return sent_to(o_block(b, h), send, o_recv.at[b, h], (me, to))

    segs = Line(lambda b: SEG.at[b], s_recv, s_send, seq)
    ws = Line(lambda b: W.at[pl.ds(pl.multiple_of(b * deep, 16), deep)], w_recv, w_send, seq)
    kvs = Line(lambda b: KV.at[b], k_recv, k_send, seq, down=False)
    wos = Line(lambda b: o_block(b, head), o_recv.at[:, head], o_send, seq)

    def share(b):
        for d, mate in enumerate(mates):
            o_copy(b, head, mate, o_y.at[d, b]).start()
        o_copy(b, head, partner, o_core.at[b, y]).start()

    def begin(stream):
        stream.up(me)
        stream.below(me)
        stream.across(me)

    begin(segs)
    for d, mate in enumerate(mates):
        x_copy(head, mate, x_send.at[d]).start()
    x_copy(head, partner, x_core.at[y]).start()
    begin(ws)
    share(me)

    def onset(k):
        @pl.when(z == k)
        def _():
            wos.up(me)

        @pl.when(line - 1 - z == k)
        def _():
            wos.below(me)

    onset(0)
    for move in small:
        move.wait()
    for mate in mates:
        x_copy(mate, partner, x_core.at[mate // 2]).wait_recv()
        x_copy(mate, partner, x_core.at[mate // 2]).start()
    segs.step(1)
    ws.step(1)
    onset(1)
    for other in range(ys):
        x_copy(2 * other + 1 - core, partner, x_core.at[other]).wait_recv()

    half = rows // 2

    def norm_rows(r, _):
        at = pl.ds(pl.multiple_of(r * half, half), half)
        total = jnp.zeros((half, 1), F32)
        for h in range(heads):
            wide = X[h, at, :].astype(F32)
            total += jnp.sum(wide * wide, axis=1, keepdims=True)
        scale = lax.rsqrt(total / width + EPS)
        for h in range(heads):
            gain = pre[0:1, h * cut : (h + 1) * cut]
            XN[h, at, :] = (X[h, at, :].astype(F32) * scale * gain).astype(BF16)
        return 0

    lax.fori_loop(0, 2, norm_rows, 0)
    for k in range(2, line):
        segs.step(k)
        ws.step(k)
        onset(k)
    wos.across(me)
    segs.pairs()
    own = jnp.broadcast_to(SEG[me].astype(F32), (HD, rows))
    col = jnp.transpose(own)[:, 0:1]
    start = jnp.zeros((rows, 1), F32)
    for j in range(seq):
        start += jnp.sum((SEG[j].astype(F32) < col).astype(F32), axis=1, keepdims=True)
    index = (me * rows + lax.broadcasted_iota(jnp.int32, (rows, 1), 0)).astype(F32)
    angle = (index - start) * freq[...]
    cosine = jnp.cos(angle)
    sine = jnp.sin(angle)
    lane = lax.broadcasted_iota(jnp.int32, (rows, HD), 1)
    sine = jnp.where(lane < HD // 2, -sine, sine)
    wos.near(1, share)
    ws.pairs()

    ACC[...] = jnp.zeros_like(ACC)

    def project(h, _):
        part = W[pl.ds(pl.multiple_of(h * cut, 128), cut), :]
        ACC[...] += jnp.dot(XN[h], part, preferred_element_type=F32)
        return 0

    lax.fori_loop(0, heads, project, 0)

    def turn(values):
        return values * cosine + pltpu.roll(values, HD // 2, 1) * sine

    for g in range(GROUP):
        RQ[g * rows : (g + 1) * rows, :] = (
            turn(ACC[:, g * HD : (g + 1) * HD]) * SCALAR ** (-0.5)
        ).astype(BF16)
    KV[me, :, 0:HD] = turn(ACC[:, qd : qd + HD]).astype(BF16)
    KV[me, :, HD : 2 * HD] = ACC[:, qd + kd : qd + kd + HD].astype(BF16)
    begin(kvs)
    wos.pairs(share, 0, 1)
    for k in range(1, line):
        if k + 1 < line:
            wos.near(k + 1, share)
        kvs.step(k)
        wos.far(k)
    kvs.pairs()

    start2 = jnp.concatenate([start] * GROUP, axis=0)
    index2 = jnp.concatenate([index] * GROUP, axis=0)
    NUM[...] = jnp.zeros_like(NUM)
    DEN[...] = jnp.zeros_like(DEN)

    def attend(j, _):
        s = lax.dot_general(
            RQ[...], KV[j, :, 0:HD], (((1,), (1,)), ((), ())), preferred_element_type=F32
        )
        at = (j * rows + lax.broadcasted_iota(jnp.int32, (1, rows), 1)).astype(F32)
        p = jnp.where(
            (at >= start2) & (at <= index2), jnp.exp(CAP * jnp.tanh(s * (1.0 / CAP))), 0.0
        )
        DEN[...] += jnp.sum(p, axis=1, keepdims=True)
        NUM[...] += jnp.dot(p.astype(BF16), KV[j, :, HD : 2 * HD], preferred_element_type=F32)
        return 0

    lax.fori_loop(0, me + 1, attend, 0)
    ratio = (NUM[...] / DEN[:, 0:1]).astype(BF16)
    for g in range(GROUP):
        ATT[head, :, g * HD : (g + 1) * HD] = ratio[g * rows : (g + 1) * rows, :]
    for d, mate in enumerate(mates):
        a_copy(head, mate, a_send.at[d]).start()
    a_copy(head, partner, a_core.at[y]).start()

    wos.pairs(share, 1)
    for mate in mates:
        a_copy(mate, partner, a_core.at[mate // 2]).wait_recv()
        a_copy(mate, partner, a_core.at[mate // 2]).start()
    for b in range(seq):
        for mate in mates:
            o_copy(b, mate, partner, o_core.at[b, mate // 2]).wait_recv()
            o_copy(b, mate, partner, o_core.at[b, mate // 2]).start()
    for other in range(ys):
        a_copy(2 * other + 1 - core, partner, a_core.at[other]).wait_recv()
    for b in range(seq):
        for other in range(ys):
            o_copy(b, 2 * other + 1 - core, partner, o_core.at[b, other]).wait_recv()

    def emit(n, total):
        acc = jnp.zeros((rows, cut), F32)
        at = pl.ds(pl.multiple_of(n * cut, 128), cut)
        for h in range(heads):
            part = lax.dot_general(
                ATT[h], WO[h, at, :], (((1,), (1,)), ((), ())), preferred_element_type=F32
            )
            acc += part.astype(BF16).astype(F32)
        PR[n] = acc
        return total + jnp.sum(acc * acc, axis=1, keepdims=True)

    total = lax.fori_loop(0, heads, emit, jnp.zeros((rows, 1), F32))
    scale = lax.rsqrt(total / width + EPS)

    def finish(h, _):
        at = pl.ds(pl.multiple_of(h * cut, 128), cut)
        out[:, at] = (X[h].astype(F32) + PR[h] * scale * post[0:1, at]).astype(BF16)
        return 0

    lax.fori_loop(0, heads, finish, 0)

    for stream in (segs, ws, kvs, wos):
        stream.drain()
    for d, mate in enumerate(mates):
        x_copy(head, mate, x_send.at[d]).wait_send()
        a_copy(head, mate, a_send.at[d]).wait_send()
    for other in range(ys):
        x_copy(2 * other + core, partner, x_core.at[other]).wait_send()
        a_copy(2 * other + core, partner, a_core.at[other]).wait_send()
    for b in range(seq):
        for d, mate in enumerate(mates):
            o_copy(b, head, mate, o_y.at[d, b]).wait_send()
        for other in range(ys):
            o_copy(b, 2 * other + core, partner, o_core.at[b, other]).wait_send()


def fused(tokens, segments, pre_gain, post_gain, w_query, w_key, w_value, w_out):
    seq, heads = lax.axis_size("seq"), lax.axis_size("head")
    rows, cut = tokens.shape
    width = cut * heads
    deep = width // seq
    qd, kd = w_query.shape[1], w_key.shape[1]
    half = HD // 2
    freq = np.float32(10000.0) ** (-(np.arange(half, dtype=np.float32) / np.float32(half)))
    freq = np.concatenate([freq, freq])[None, :].astype(np.float32)
    hbm = pl.BlockSpec(memory_space=pl.ANY)
    vmem = pl.BlockSpec(memory_space=pltpu.VMEM)
    dma = pltpu.SemaphoreType.DMA
    ys = heads // 2
    return pl.pallas_call(
        functools.partial(kernel, seq, heads, rows, width),
        out_shape=jax.ShapeDtypeStruct((rows, width), BF16),
        in_specs=[hbm] * 9,
        out_specs=vmem,
        scratch_shapes=[
            pltpu.VMEM((heads, rows, cut), BF16),
            pltpu.VMEM((heads, rows, cut), BF16),
            pltpu.VMEM((width, qd + 2 * kd), BF16),
            pltpu.VMEM((heads, width, w_out.shape[0]), BF16),
            pltpu.VMEM((seq, 1, rows), jnp.int32),
            pltpu.VMEM((seq, rows, 2 * HD), BF16),
            pltpu.VMEM((heads, rows, GROUP * HD), BF16),
            pltpu.VMEM((heads, rows, cut), F32),
            pltpu.VMEM((rows, qd + 2 * kd), F32),
            pltpu.VMEM((GROUP * rows, HD), BF16),
            pltpu.VMEM((GROUP * rows, HD), F32),
            pltpu.VMEM((GROUP * rows, HD), F32),
            pltpu.VMEM((1, width), F32),
            pltpu.VMEM((1, width), F32),
            pltpu.VMEM((1, HD), F32),
            dma((9,)),
            dma((heads,)), dma((max(ys - 1, 1),)), dma((ys,)),
            dma((seq,)), dma((3, seq)),
            dma((seq,)), dma((3, seq)),
            dma((seq, heads)), dma((3, seq)), dma((max(ys - 1, 1), seq)), dma((seq, ys)),
            dma((seq,)), dma((3, seq)),
            dma((heads,)), dma((max(ys - 1, 1),)), dma((ys,)),
        ],
        compiler_params=pltpu.CompilerParams(
            collective_id=0, has_side_effects=True, vmem_limit_bytes=60 * 2**20
        ),
    )(
        tokens, segments[None, :], w_query, w_key, w_value, w_out.T,
        pre_gain[None, :], post_gain[None, :], freq,
    )


def solution(mesh):
    specs = (
        P("seq", "head"),
        P("seq"),
        P(),
        P(),
        P("seq", "head"),
        P("seq", "head"),
        P("seq", "head"),
        P("head", "seq"),
    )

    def run(*args):
        small = fits(mesh, args[0].shape, args[5].shape, args[7].shape)
        return jax.shard_map(
            fused if small else local,
            mesh=mesh,
            in_specs=specs,
            out_specs=P("seq", None),
            check_vma=False,
        )(*args)

    return run
```

```python
import functools

import jax
import jax.numpy as jnp
import numpy as np
from jax import lax
from jax.experimental import pallas as pl
from jax.experimental.pallas import tpu as pltpu
from jax.sharding import PartitionSpec as P

HD = 128
GROUP = 2
SCALAR = 144
DOCS = 8


EPS = 1e-06
CAP = 50.0


def carried_in(value, axis, join, neutral):
    count, mine = (lax.axis_size(axis), lax.axis_index(axis))
    pieces = lax.all_gather(value, axis)
    subtotal = jnp.full_like(value, 0) + jnp.asarray(neutral, value.dtype)

    def step(position, subtotal):
        longer = join(subtotal, pieces[position])
        return jnp.where(position < mine, longer, subtotal)

    return lax.fori_loop(0, count - 1, step, subtotal)


def rotate(values, position, width):
    count = values.shape[1] // width
    half = width // 2
    shaped = values.reshape(values.shape[0], count, width)
    freq = 10000.0 ** (-(jnp.arange(half, dtype=jnp.float32) / half))
    angle = position[:, None] * freq[None, :]
    cosine = jnp.cos(angle)[:, None, :]
    sine = jnp.sin(angle)[:, None, :]
    first = shaped[:, :, :half]
    second = shaped[:, :, half:]
    turned = jnp.concatenate(
        [first * cosine - second * sine, second * cosine + first * sine], axis=2
    )
    return turned.reshape(values.shape[0], count * width)


def add_counts(earlier, later):
    return earlier + later


def local(tokens, segments, pre_gain, post_gain, w_query, w_key, w_value, w_out):
    rows = tokens.shape[0]
    whole = lax.all_gather(tokens, "head", axis=1, tiled=True)
    wide = whole.astype(jnp.float32)
    normed = (
        wide * lax.rsqrt(jnp.mean(wide * wide, axis=1, keepdims=True) + EPS) * pre_gain
    ).astype(jnp.bfloat16)
    pieces = (
        lax.all_gather(w_query, "seq", axis=0, tiled=True),
        lax.all_gather(w_key, "seq", axis=0, tiled=True),
        lax.all_gather(w_value, "seq", axis=0, tiled=True),
    )
    query, key_proj, value_proj = tuple(
        (jnp.dot(normed, piece, preferred_element_type=jnp.float32) for piece in pieces)
    )
    levels = jnp.arange(DOCS, dtype=jnp.int32)
    below = jnp.sum((levels[None, :] > segments[:, None]).astype(jnp.float32), axis=0)
    earlier = carried_in(below, "seq", add_counts, jnp.zeros((DOCS,), jnp.float32))
    starts = earlier + below
    onehot = (segments[:, None] == levels[None, :]).astype(jnp.float32)
    tok_start = jnp.sum(onehot * starts[None, :], axis=1)
    offset = lax.axis_index("seq") * rows
    index_f = (offset + jnp.arange(rows, dtype=jnp.int32)).astype(jnp.float32)
    position = index_f - tok_start
    kv_count = w_key.shape[1] // HD
    rq = (rotate(query, position, HD) * SCALAR ** (-0.5)).astype(jnp.bfloat16)
    rk = rotate(key_proj, position, HD).astype(jnp.bfloat16)
    vb = value_proj.astype(jnp.bfloat16)
    stacked = (
        rq.reshape(rows, kv_count, GROUP, HD)
        .transpose(1, 2, 0, 3)
        .reshape(kv_count, GROUP * rows, HD)
    )
    query_start = jnp.tile(tok_start, GROUP)
    query_index = jnp.tile(index_f, GROUP)
    empty = (
        jnp.zeros((kv_count, GROUP * rows, HD), jnp.float32),
        jnp.zeros((kv_count, GROUP * rows), jnp.float32),
    )
    keys_all = lax.all_gather(rk, "seq", axis=0, tiled=True)
    values_all = lax.all_gather(vb, "seq", axis=0, tiled=True)
    count = keys_all.shape[0]
    block = 1024
    steps_total = count // block

    def compute(offset_blk, state):
        numer, denom = state
        keys_blk = lax.dynamic_slice_in_dim(keys_all, offset_blk, block, 0).reshape(
            block, kv_count, HD
        )
        values_blk = lax.dynamic_slice_in_dim(values_all, offset_blk, block, 0).reshape(
            block, kv_count, HD
        )
        key_index = (offset_blk + jnp.arange(block, dtype=jnp.int32)).astype(jnp.float32)
        scores = jnp.einsum("cqd,kcd->cqk", stacked, keys_blk, preferred_element_type=jnp.float32)
        capped = CAP * jnp.tanh(scores / CAP)
        allowed = (key_index[None, None, :] >= query_start[None, :, None]) & (
            key_index[None, None, :] <= query_index[None, :, None]
        )
        weights = jnp.where(allowed, jnp.exp(capped), 0.0)
        numer = numer + jnp.einsum(
            "cqk,kcd->cqd",
            weights.astype(jnp.bfloat16),
            values_blk,
            preferred_element_type=jnp.float32,
        )
        denom = denom + jnp.sum(weights, axis=2)
        return (numer, denom)

    def one_block(step, state):
        offset_blk = step * block
        return compute(offset_blk, state)

    numer, denom = lax.fori_loop(0, steps_total, one_block, empty)
    attn = (numer / denom[:, :, None]).reshape(kv_count, GROUP, rows, HD).transpose(2, 0, 1, 3)
    attn = attn.reshape(rows, kv_count * GROUP * HD).astype(jnp.bfloat16)
    partial_proj = jnp.dot(
        attn, lax.all_gather(w_out, "seq", axis=1, tiled=True), preferred_element_type=jnp.float32
    )
    partial_proj = lax.optimization_barrier(partial_proj.astype(jnp.bfloat16)).astype(jnp.float32)
    summed = lax.psum(partial_proj.astype(jnp.bfloat16), "head").astype(jnp.float32)
    scale = lax.rsqrt(jnp.mean(summed * summed, axis=1, keepdims=True) + EPS)
    return (wide + summed * scale * post_gain).astype(jnp.bfloat16)


MESH = pl.DeviceIdType.MESH
BF16 = jnp.bfloat16
F32 = jnp.float32


def fits(mesh, tokens, w_key, w_out):
    seq, head = mesh.shape["seq"], mesh.shape["head"]
    width = tokens[1]
    weights = 2 * width * (w_key[1] // head) * (GROUP + 2)
    outs = 2 * w_out[0] * width
    rows = tokens[0] // seq
    rest = rows * width * (2 + 2 + 4 + 2) + tokens[0] * (w_key[1] // head) * 4
    return (
        seq % 2 == 0
        and seq > 2
        and head % 2 == 0
        and seq % (2 * head) == 0
        and w_key[1] // head == HD
        and (width // head) % 128 == 0
        and weights + outs + rest < 40 * 2**20
    )


class Line:
    def __init__(self, ref, recv, send, seq, down=True):
        self.ref, self.recv, self.send, self.down = ref, recv, send, down
        self.count = seq // 2
        me = lax.axis_index("seq")
        self.z, self.x = me // 2, lax.rem(me, 2)
        self.head = lax.axis_index("head")
        self.me = me

    def copy(self, block, way):
        target = (
            2 * (self.z + 1) + self.x,
            2 * (self.z - 1) + self.x,
            2 * self.z + 1 - self.x,
        )[way]
        return pltpu.make_async_remote_copy(
            src_ref=self.ref(block),
            dst_ref=self.ref(block),
            send_sem=self.send.at[way, block],
            recv_sem=self.recv.at[block],
            device_id=(target, self.head),
            device_id_type=MESH,
        )

    def up(self, block):
        @pl.when(self.z < self.count - 1)
        def _():
            self.copy(block, 0).start()

    def below(self, block):
        if self.down:

            @pl.when(self.z > 0)
            def _():
                self.copy(block, 1).start()

    def across(self, block):
        self.copy(block, 2).start()

    def wait(self, block):
        self.copy(block, 2).wait_recv()

    def at(self, k, act):
        @pl.when(self.z - k >= 0)
        def _():
            act(2 * (self.z - k) + self.x, self.up)

        if self.down:

            @pl.when(self.z + k < self.count)
            def _():
                act(2 * (self.z + k) + self.x, self.below)

    def near(self, k, also):
        def act(block, onward):
            self.wait(block)
            onward(block)
            also(block)

        self.at(k, act)

    def far(self, k):
        self.at(k, lambda block, onward: self.across(block))

    def step(self, k):
        self.near(k, self.across)

    def pairs(self, also=None, first=0, last=None):
        for away in range(first, self.count if last is None else last):
            z = lax.rem(self.z + away, self.count)
            block = 2 * z + 1 - self.x

            def take():
                self.wait(block)
                if also is not None:
                    also(block)

            if self.down:
                take()
            else:
                pl.when(z <= self.z)(take)

    def drain(self):
        for z in range(self.count):
            block = 2 * z + self.x

            def sent():
                self.copy(block, 2).wait_send()

            if self.down:
                sent()

                @pl.when((self.z > 0) & (z >= self.z))
                def _():
                    self.copy(block, 1).wait_send()
            else:
                pl.when(z <= self.z)(sent)

            @pl.when((self.z < self.count - 1) & (z <= self.z))
            def _():
                self.copy(block, 0).wait_send()


def kernel(
    seq, heads, rows, width,
    tok, seg_row, wq, wk, wv, wo_in, pre_in, post_in, freq_in,
    out,
    X, XN, W, WO, SEG, KV, ATT, PR, ACC, RQ, NUM, DEN, pre, post, freq,
    loc, x_recv, x_send, x_core, s_recv, s_send, w_recv, w_send,
    o_recv, o_send, o_y, o_core, k_recv, k_send, a_recv, a_send, a_core,
):
    me, head = lax.axis_index("seq"), lax.axis_index("head")
    z, x = me // 2, lax.rem(me, 2)
    y, core = head // 2, lax.rem(head, 2)
    ys, line = heads // 2, seq // 2
    partner = 2 * y + 1 - core
    deep = width // seq
    cut = width // heads
    mates = [2 * lax.rem(y + d, ys) + core for d in range(1, ys)]

    moves = [
        pltpu.make_async_copy(seg_row, SEG.at[me], loc.at[0]),
        pltpu.make_async_copy(tok, X.at[head], loc.at[1]),
    ]
    mine = W.at[pl.ds(pl.multiple_of(me * deep, 16), deep)]
    kd = wk.shape[1]
    qd = wq.shape[1]
    moves += [
        pltpu.make_async_copy(wq, mine.at[:, pl.ds(0, qd)], loc.at[2]),
        pltpu.make_async_copy(wk, mine.at[:, pl.ds(qd, kd)], loc.at[3]),
        pltpu.make_async_copy(wv, mine.at[:, pl.ds(qd + kd, kd)], loc.at[4]),
        pltpu.make_async_copy(
            wo_in, WO.at[head, pl.ds(pl.multiple_of(me * deep, 16), deep)], loc.at[5]
        ),
    ]
    small = [
        pltpu.make_async_copy(pre_in, pre, loc.at[6]),
        pltpu.make_async_copy(post_in, post, loc.at[7]),
        pltpu.make_async_copy(freq_in, freq, loc.at[8]),
    ]
    for move in small:
        move.start()
    for move in moves:
        move.start()

    barrier = pltpu.get_barrier_semaphore()

    def greet(where):
        pl.semaphore_signal(barrier, inc=1, device_id=where, device_id_type=MESH)

    greet((2 * z + 1 - x, head))
    greet((me, partner))
    for mate in mates:
        greet((me, mate))

    @pl.when(z > 0)
    def _():
        greet((me - 2, head))

    @pl.when(z < line - 1)
    def _():
        greet((me + 2, head))

    ends = (z > 0).astype(jnp.int32) + (z < line - 1).astype(jnp.int32)
    pl.semaphore_wait(barrier, 2 + len(mates) + ends)

    for move in moves:
        move.wait()

    def sent_to(ref, send, recv, where):
        return pltpu.make_async_remote_copy(
            src_ref=ref, dst_ref=ref, send_sem=send, recv_sem=recv,
            device_id=where, device_id_type=MESH,
        )

    def x_copy(h, to, send):
        return sent_to(X.at[h], send, x_recv.at[h], (me, to))

    def a_copy(h, to, send):
        return sent_to(ATT.at[h], send, a_recv.at[h], (me, to))

    def o_block(b, h):
        return WO.at[h, pl.ds(pl.multiple_of(b * deep, 16), deep)]

    def o_copy(b, h, to, send):
        return sent_to(o_block(b, h), send, o_recv.at[b, h], (me, to))

    segs = Line(lambda b: SEG.at[b], s_recv, s_send, seq)
    ws = Line(lambda b: W.at[pl.ds(pl.multiple_of(b * deep, 16), deep)], w_recv, w_send, seq)
    kvs = Line(lambda b: KV.at[b], k_recv, k_send, seq, down=False)
    wos = Line(lambda b: o_block(b, head), o_recv.at[:, head], o_send, seq)

    def share(b):
        for d, mate in enumerate(mates):
            o_copy(b, head, mate, o_y.at[d, b]).start()
        o_copy(b, head, partner, o_core.at[b, y]).start()

    def begin(stream):
        stream.up(me)
        stream.below(me)
        stream.across(me)

    begin(segs)
    for d, mate in enumerate(mates):
        x_copy(head, mate, x_send.at[d]).start()
    x_copy(head, partner, x_core.at[y]).start()
    begin(ws)
    share(me)

    def onset(k):
        @pl.when(z == k)
        def _():
            wos.up(me)

        @pl.when(line - 1 - z == k)
        def _():
            wos.below(me)

    onset(0)
    for move in small:
        move.wait()
    for mate in mates:
        x_copy(mate, partner, x_core.at[mate // 2]).wait_recv()
        x_copy(mate, partner, x_core.at[mate // 2]).start()
    segs.step(1)
    ws.step(1)
    onset(1)
    for other in range(ys):
        x_copy(2 * other + 1 - core, partner, x_core.at[other]).wait_recv()

    half = rows // 2

    def norm_rows(r, _):
        at = pl.ds(pl.multiple_of(r * half, half), half)
        total = jnp.zeros((half, 1), F32)
        for h in range(heads):
            wide = X[h, at, :].astype(F32)
            total += jnp.sum(wide * wide, axis=1, keepdims=True)
        scale = lax.rsqrt(total / width + EPS)
        for h in range(heads):
            gain = pre[0:1, h * cut : (h + 1) * cut]
            XN[h, at, :] = (X[h, at, :].astype(F32) * scale * gain).astype(BF16)
        return 0

    lax.fori_loop(0, 2, norm_rows, 0)
    for k in range(2, line):
        segs.step(k)
        ws.step(k)
        onset(k)
    wos.across(me)
    segs.pairs()
    own = jnp.broadcast_to(SEG[me].astype(F32), (HD, rows))
    col = jnp.transpose(own)[:, 0:1]
    start = jnp.zeros((rows, 1), F32)
    for j in range(seq):
        start += jnp.sum((SEG[j].astype(F32) < col).astype(F32), axis=1, keepdims=True)
    index = (me * rows + lax.broadcasted_iota(jnp.int32, (rows, 1), 0)).astype(F32)
    angle = (index - start) * freq[...]
    cosine = jnp.cos(angle)
    sine = jnp.sin(angle)
    lane = lax.broadcasted_iota(jnp.int32, (rows, HD), 1)
    sine = jnp.where(lane < HD // 2, -sine, sine)
    wos.near(1, share)
    ws.pairs()

    ACC[...] = jnp.zeros_like(ACC)

    def project(h, _):
        part = W[pl.ds(pl.multiple_of(h * cut, 128), cut), :]
        ACC[...] += jnp.dot(XN[h], part, preferred_element_type=F32)
        return 0

    lax.fori_loop(0, heads, project, 0)

    def turn(values):
        return values * cosine + pltpu.roll(values, HD // 2, 1) * sine

    for g in range(GROUP):
        RQ[g * rows : (g + 1) * rows, :] = (
            turn(ACC[:, g * HD : (g + 1) * HD]) * SCALAR ** (-0.5)
        ).astype(BF16)
    KV[me, :, 0:HD] = turn(ACC[:, qd : qd + HD]).astype(BF16)
    KV[me, :, HD : 2 * HD] = ACC[:, qd + kd : qd + kd + HD].astype(BF16)
    wos.far(1)
    begin(kvs)
    wos.pairs(share, 0, 1)
    for k in range(1, line):
        if k + 1 < line:
            wos.near(k + 1, share)
        kvs.step(k)
        if k > 1:
            wos.far(k)
    kvs.pairs()

    start2 = jnp.concatenate([start] * GROUP, axis=0)
    index2 = jnp.concatenate([index] * GROUP, axis=0)
    NUM[...] = jnp.zeros_like(NUM)
    DEN[...] = jnp.zeros_like(DEN)

    def attend(j, _):
        s = lax.dot_general(
            RQ[...], KV[j, :, 0:HD], (((1,), (1,)), ((), ())), preferred_element_type=F32
        )
        at = (j * rows + lax.broadcasted_iota(jnp.int32, (1, rows), 1)).astype(F32)
        p = jnp.where(
            (at >= start2) & (at <= index2), jnp.exp(CAP * jnp.tanh(s * (1.0 / CAP))), 0.0
        )
        DEN[...] += jnp.sum(p, axis=1, keepdims=True)
        NUM[...] += jnp.dot(p.astype(BF16), KV[j, :, HD : 2 * HD], preferred_element_type=F32)
        return 0

    lax.fori_loop(0, me + 1, attend, 0)
    ratio = (NUM[...] / DEN[:, 0:1]).astype(BF16)
    for g in range(GROUP):
        ATT[head, :, g * HD : (g + 1) * HD] = ratio[g * rows : (g + 1) * rows, :]
    for d, mate in enumerate(mates):
        a_copy(head, mate, a_send.at[d]).start()
    a_copy(head, partner, a_core.at[y]).start()

    group = line // heads
    nest = z // group
    less = jnp.minimum(nest, heads - 1 - nest)
    low = (nest <= heads - 1 - nest).astype(jnp.int32)

    def nearest(i):
        near = (i <= 2 * less).astype(jnp.int32)
        beside = nest + ((i + 1) // 2) * (1 - 2 * (i % 2))
        past = low * i + (1 - low) * (heads - 1 - i)
        return near * beside + (1 - near) * past

    for i in range(heads):
        for t in range(group):
            there = nearest(i) * group + t
            block = 2 * there + 1 - x

            @pl.when(there != z)
            def _():
                wos.wait(block)
                share(block)

    for mate in mates:
        a_copy(mate, partner, a_core.at[mate // 2]).wait_recv()
        a_copy(mate, partner, a_core.at[mate // 2]).start()
    for other in range(ys):
        a_copy(2 * other + 1 - core, partner, a_core.at[other]).wait_recv()

    total = jnp.zeros((rows, 1), F32)
    for i in range(heads):
        n = nearest(i)
        for j in range(2 * group):
            b = 2 * n * group + j
            for mate in mates:
                o_copy(b, mate, partner, o_core.at[b, mate // 2]).wait_recv()
                o_copy(b, mate, partner, o_core.at[b, mate // 2]).start()
        for j in range(2 * group):
            b = 2 * n * group + j
            for other in range(ys):
                o_copy(b, 2 * other + 1 - core, partner, o_core.at[b, other]).wait_recv()
        at = pl.ds(pl.multiple_of(n * cut, 128), cut)

        def emit(r, _):
            some = pl.ds(pl.multiple_of(r * half, half), half)
            acc = jnp.zeros((half, cut), F32)
            for h in range(heads):
                part = lax.dot_general(
                    ATT[h, some, :], WO[h, at, :], (((1,), (1,)), ((), ())),
                    preferred_element_type=F32,
                )
                acc += part.astype(BF16).astype(F32)
            PR[n, some, :] = acc
            return 0

        lax.fori_loop(0, 2, emit, 0)
        total += jnp.sum(PR[n] * PR[n], axis=1, keepdims=True)
    scale = lax.rsqrt(total / width + EPS)

    def finish(h, _):
        at = pl.ds(pl.multiple_of(h * cut, 128), cut)
        out[:, at] = (X[h].astype(F32) + PR[h] * scale * post[0:1, at]).astype(BF16)
        return 0

    lax.fori_loop(0, heads, finish, 0)

    for stream in (segs, ws, kvs, wos):
        stream.drain()
    for d, mate in enumerate(mates):
        x_copy(head, mate, x_send.at[d]).wait_send()
        a_copy(head, mate, a_send.at[d]).wait_send()
    for other in range(ys):
        x_copy(2 * other + core, partner, x_core.at[other]).wait_send()
        a_copy(2 * other + core, partner, a_core.at[other]).wait_send()
    for b in range(seq):
        for d, mate in enumerate(mates):
            o_copy(b, head, mate, o_y.at[d, b]).wait_send()
        for other in range(ys):
            o_copy(b, 2 * other + core, partner, o_core.at[b, other]).wait_send()


def fused(tokens, segments, pre_gain, post_gain, w_query, w_key, w_value, w_out):
    seq, heads = lax.axis_size("seq"), lax.axis_size("head")
    rows, cut = tokens.shape
    width = cut * heads
    deep = width // seq
    qd, kd = w_query.shape[1], w_key.shape[1]
    half = HD // 2
    freq = np.float32(10000.0) ** (-(np.arange(half, dtype=np.float32) / np.float32(half)))
    freq = np.concatenate([freq, freq])[None, :].astype(np.float32)
    hbm = pl.BlockSpec(memory_space=pl.ANY)
    vmem = pl.BlockSpec(memory_space=pltpu.VMEM)
    dma = pltpu.SemaphoreType.DMA
    ys = heads // 2
    return pl.pallas_call(
        functools.partial(kernel, seq, heads, rows, width),
        out_shape=jax.ShapeDtypeStruct((rows, width), BF16),
        in_specs=[hbm] * 9,
        out_specs=vmem,
        scratch_shapes=[
            pltpu.VMEM((heads, rows, cut), BF16),
            pltpu.VMEM((heads, rows, cut), BF16),
            pltpu.VMEM((width, qd + 2 * kd), BF16),
            pltpu.VMEM((heads, width, w_out.shape[0]), BF16),
            pltpu.VMEM((seq, 1, rows), jnp.int32),
            pltpu.VMEM((seq, rows, 2 * HD), BF16),
            pltpu.VMEM((heads, rows, GROUP * HD), BF16),
            pltpu.VMEM((heads, rows, cut), F32),
            pltpu.VMEM((rows, qd + 2 * kd), F32),
            pltpu.VMEM((GROUP * rows, HD), BF16),
            pltpu.VMEM((GROUP * rows, HD), F32),
            pltpu.VMEM((GROUP * rows, HD), F32),
            pltpu.VMEM((1, width), F32),
            pltpu.VMEM((1, width), F32),
            pltpu.VMEM((1, HD), F32),
            dma((9,)),
            dma((heads,)), dma((max(ys - 1, 1),)), dma((ys,)),
            dma((seq,)), dma((3, seq)),
            dma((seq,)), dma((3, seq)),
            dma((seq, heads)), dma((3, seq)), dma((max(ys - 1, 1), seq)), dma((seq, ys)),
            dma((seq,)), dma((3, seq)),
            dma((heads,)), dma((max(ys - 1, 1),)), dma((ys,)),
        ],
        compiler_params=pltpu.CompilerParams(
            collective_id=0, has_side_effects=True, vmem_limit_bytes=60 * 2**20
        ),
    )(
        tokens, segments[None, :], w_query, w_key, w_value, w_out.T,
        pre_gain[None, :], post_gain[None, :], freq,
    )


def solution(mesh):
    specs = (
        P("seq", "head"),
        P("seq"),
        P(),
        P(),
        P("seq", "head"),
        P("seq", "head"),
        P("seq", "head"),
        P("head", "seq"),
    )

    def run(*args):
        small = fits(mesh, args[0].shape, args[5].shape, args[7].shape)
        return jax.shard_map(
            fused if small else local,
            mesh=mesh,
            in_specs=specs,
            out_specs=P("seq", None),
            check_vma=False,
        )(*args)

    return run
```
